32 devices in a mesh: gz: 2 (over core), dp: 16 (over z, y, x).
Axes of the slice: x: 2, y: 2, z: 4, core: 2. Of those that a mesh axis runs over, the one named last changes fastest.
Arguments:
- inputs: bfloat16 [16, 32, 16, 8, 128], P('dp', None, 'gz'), may hold values from -6 to 6
- kernel_one: bfloat16 [32, 32, 3, 3, 3], replicated, may hold values from -0.21875 to 0.21875
- kernel_two: bfloat16 [32, 32, 3, 3, 3], replicated, may hold values from -0.21875 to 0.21875
- cotangent: bfloat16 [16, 32, 16, 8, 128], P('dp', None, 'gz'), may hold values from -12 to 12
Outputs:
- input_grad: bfloat16 [16, 32, 16, 8, 128], P('dp', None, 'gz')
- kernel_one_grad: float32 [32, 32, 3, 3, 3], replicated
- kernel_two_grad: float32 [32, 32, 3, 3, 3], replicated
The draws below stay inside these ranges and needn't reach their ends.
All inputs are finite; a program needn't handle non-finite values.
Results may differ from the reference program's by a relative error of at most 0.006.
Values may be sent and summed in bfloat16 or wider, within the bound.
A program may use at most 64 MiB of HBM per device.

```python
import math
import jax
import jax.numpy as jnp
from jax import lax

C = 32
NY = 8
NX = 128
NZ = 16
BATCH = 16


def draw_cotangent(key, part):
    sample_pos = jnp.arange(BATCH, dtype=jnp.float32) / max(BATCH - 1, 1)
    plane_pos = jnp.arange(NZ, dtype=jnp.float32) / max(NZ - 1, 1)
    scale = 1.0 + sample_pos[:, None, None, None, None] + plane_pos[None, None, :, None, None]
    base = jnp.clip(jax.random.normal(key, (BATCH, C, NZ, NY, NX), jnp.float32), -4.0, 4.0)
    return (base * scale).astype(jnp.bfloat16)


def steps_of(stream_key, extent, split, low, high):
    def one(position, parts):
        draws = jax.random.uniform(jax.random.fold_in(jax.random.fold_in(stream_key, 6), position), (parts,), jnp.float32, low / len(split), high / len(split))
        return jnp.repeat(jnp.exp(draws), extent[position] // parts).reshape((-1,) + (1,) * (len(extent) - position - 1))

    gain = one(*split[0])
    for cut in split[1:]:
        gain = gain * one(*cut)
    return gain


def normal_values(rng, extent, spread, most, pieces=(), held_as=jnp.bfloat16):
    entries = spread * jax.random.normal(rng, extent, jnp.float32)
    if pieces:
        entries = entries * steps_of(rng, extent, pieces, -0.22, 0.18)
    return jnp.clip(entries, -most, most).astype(held_as)


def setup_inputs(seed: int = 0) -> dict:
    streams_of = jax.random.split(jax.random.key(seed), 5)
    return {
        "inputs": normal_values(streams_of[0], (BATCH, C, NZ, NY, NX), 1.0, 6.0, ((0, 16), (2, 2))),
        "kernel_one": normal_values(streams_of[1], (C, C, 3, 3, 3), (27 * C) ** -0.5, 0.21875),
        "kernel_two": normal_values(streams_of[2], (C, C, 3, 3, 3), (27 * C) ** -0.5, 0.21875),
        "cotangent": draw_cotangent(jax.random.fold_in(streams_of[4], 71), 0),
    }


def convolve(field, kernel):
    out = lax.conv_general_dilated(field[None], kernel, (1, 1, 1), ((1, 1), (1, 1), (1, 1)), dimension_numbers=('NCDHW', 'OIDHW', 'NCDHW'), preferred_element_type=jnp.float32)
    return out[0]

def flipped(kernel):
    return jnp.swapaxes(jnp.flip(kernel, (2, 3, 4)), 0, 1)

def kernel_terms(padded, grad):
    out = lax.conv_general_dilated(padded[None], grad[None], (1, 1, 1), 'VALID', dimension_numbers=('CNDHW', 'IODHW', 'NCDHW'), preferred_element_type=jnp.float32)
    return jnp.transpose(out, (1, 0, 2, 3, 4))

def dsilu(value):
    sig = jax.nn.sigmoid(value)
    return sig * (1.0 + value * (1.0 - sig))

def one_sample(pair, kernel_one, kernel_two):
    source, upstream = pair
    pre_one = convolve(source, kernel_one)
    hidden = jax.nn.silu(pre_one).astype(jnp.bfloat16)
    pre_two = convolve(hidden, kernel_two)
    grad_two = (upstream.astype(jnp.float32) * dsilu(pre_two)).astype(jnp.bfloat16)
    hidden_grad = convolve(grad_two, flipped(kernel_two))
    grad_one = (hidden_grad * dsilu(pre_one)).astype(jnp.bfloat16)
    input_grad = convolve(grad_one, flipped(kernel_one)).astype(jnp.bfloat16)
    widths = ((0, 0), (1, 1), (1, 1), (1, 1))
    term_two = kernel_terms(jnp.pad(hidden, widths), grad_two)
    term_one = kernel_terms(jnp.pad(source, widths), grad_one)
    return (input_grad, term_one, term_two)

def reference(inputs, kernel_one, kernel_two, cotangent):
    input_grad, terms_one, terms_two = lax.map(lambda pair: one_sample(pair, kernel_one, kernel_two), (inputs, cotangent))
    factor = 1.0 / math.sqrt(BATCH * NZ * NY * NX)
    return (input_grad, lax.optimization_barrier(jnp.sum(terms_one, axis=0)) * factor, lax.optimization_barrier(jnp.sum(terms_two, axis=0)) * factor)
```

```python
import functools
import math

import jax
import jax.numpy as jnp
from jax import lax
from jax.experimental import pallas as pl
from jax.experimental.pallas import tpu as pltpu
from jax.sharding import PartitionSpec as P

MESH = pl.DeviceIdType.MESH
F32 = jnp.float32
BF16 = jnp.bfloat16
TAPS = [(plane, col) for plane in range(3) for col in range(3)]
NN = (((1,), (0,)), ((), ()))
NT = (((1,), (1,)), ((), ()))
UNROLL_UP_TO = 64


def dot(a, b, dims=NN):
    return lax.dot_general(a, b, dims, preferred_element_type=F32)


def iota(shape, dim):
    return lax.broadcasted_iota(jnp.int32, shape, dim)


def one_hot(mask):
    return jnp.where(mask, 1.0, 0.0).astype(BF16)


def sigmoid(v):
    return 0.5 * jnp.tanh(0.5 * v) + 0.5


def kernel(
    sizes,
    factor,
    x_hbm,
    w1_hbm,
    w2_hbm,
    cot_hbm,
    out_ref,
    sums_ref,
    x_ref,
    w1_ref,
    w2_ref,
    cot_ref,
    s_in,
    s_hid,
    s_g2,
    s_g1,
    wcat,
    slope,
    perm,
    packed,
    arrived,
    full,
    halo_send,
    halo_recv,
    rs_send,
    rs_recv,
    ag_send,
    ag_recv,
    load_sem,
):
    gz_count, dp_count, owners = sizes
    chan, depth, height, width = x_ref.shape
    rows = chan * height
    half = height // 2
    part_rows = half * chan
    pack = 4 * chan
    count = gz_count * dp_count
    gz = lax.axis_index("gz")
    dp = lax.axis_index("dp")
    me = gz * dp_count + dp

    loads = [
        pltpu.make_async_copy(src, dst, load_sem.at[i])
        for i, (src, dst) in enumerate(
            ((w1_hbm, w1_ref), (x_hbm, x_ref), (w2_hbm, w2_ref), (cot_hbm, cot_ref))
        )
    ]
    for copy in loads:
        copy.start()

    barrier = pltpu.get_barrier_semaphore()
    quarter = max(dp_count // 4, 1)
    offsets = [(g, d) for g in range(gz_count) for d in range(dp_count) if g or d]
    offsets.sort(key=lambda o: (0, 2, 1, 2)[o[1] // quarter % 4] * -1)

    def each_peer(act):
        if count <= UNROLL_UP_TO:
            for slot, (g, d) in enumerate(offsets):
                act(slot, lax.rem(gz + g, gz_count), lax.rem(dp + d, dp_count))
        else:

            def step(k, carry):
                dev = lax.rem(me + k, count)
                act(k - 1, dev // dp_count, lax.rem(dev, dp_count))
                return carry

            lax.fori_loop(1, count, step, 0)

    def greet(slot, to_gz, to_dp):
        pl.semaphore_signal(
            barrier, inc=1, device_id={"gz": to_gz, "dp": to_dp}, device_id_type=MESH
        )

    each_peer(greet)

    slabs = (s_in, s_hid, s_g2, s_g1)

    @pl.when(gz == 0)
    def _():
        for s in slabs:
            s[:, 0] = jnp.zeros((3, rows, width), BF16)

    @pl.when(gz == gz_count - 1)
    def _():
        for s in slabs:
            s[:, depth + 1] = jnp.zeros((3, rows, width), BF16)

    r, l = iota((rows, rows), 0), iota((rows, rows), 1)
    perm[0] = one_hot((r // chan == l % height) & (r % chan == l // height))
    perm[1] = one_hot((r // height == l % chan) & (r % height == l // chan))

    lane_of = iota((part_rows, width), 1)
    not_first, not_last = lane_of != 0, lane_of != width - 1

    def put(s, p, h, value):
        at = pl.ds(h * part_rows, part_rows)
        s[1, p, at] = value.astype(BF16)
        s[0, p, at] = jnp.where(not_first, pltpu.roll(value, 1, 1), 0.0).astype(BF16)
        s[2, p, at] = jnp.where(not_last, pltpu.roll(value, width - 1, 1), 0.0).astype(BF16)

    def up_copy(n):
        return pltpu.make_async_remote_copy(
            src_ref=slabs[n].at[:, depth],
            dst_ref=slabs[n].at[:, 0],
            send_sem=halo_send.at[n, 0],
            recv_sem=halo_recv.at[n, 0],
            device_id={"gz": gz + 1, "dp": dp},
            device_id_type=MESH,
        )

    def down_copy(n):
        return pltpu.make_async_remote_copy(
            src_ref=slabs[n].at[:, 1],
            dst_ref=slabs[n].at[:, depth + 1],
            send_sem=halo_send.at[n, 1],
            recv_sem=halo_recv.at[n, 1],
            device_id={"gz": gz - 1, "dp": dp},
            device_id_type=MESH,
        )

    def send_halo(n):
        @pl.when(gz < gz_count - 1)
        def _():
            up_copy(n).start()

        @pl.when(gz > 0)
        def _():
            down_copy(n).start()

    def take_halo(n):
        @pl.when(gz > 0)
        def _():
            up_copy(n).wait_recv()

        @pl.when(gz < gz_count - 1)
        def _():
            down_copy(n).wait_recv()

    def raw(ref, p):
        return ref[:, p].astype(F32).reshape(rows, width).astype(BF16)

    edges = sorted({0, depth - 1})
    inner = [p for p in range(depth) if p not in edges]
    groups = [edges] + [inner[i : i + 2] for i in range(0, len(inner), 2)]

    def lanes(parts):
        return parts[0] if len(parts) == 1 else jnp.concatenate(parts, axis=1)

    def split(value, planes):
        return [value[:, i * width : (i + 1) * width] for i in range(len(planes))]

    def load(ref, planes):
        return split(dot(perm[0], lanes([raw(ref, p) for p in planes])), planes)

    def conv(n, s, planes, h):
        first = h * (half - 1) * chan
        span = lambda at, size: [
            lanes([s[col, p + plane, at : at + size] for p in planes]) for plane, col in TAPS
        ]
        window = jnp.concatenate(
            span(first, part_rows) + span(first + part_rows, chan), axis=0
        )
        return split(dot(wcat[n, h, :, : 9 * (part_rows + chan)], window), planes)

    lane32 = iota((chan, pack), 1)
    quad = lane32 // chan
    er, el = iota((chan, pack), 0), lane32
    eye = one_hot(iota((chan, chan), 0) == iota((chan, chan), 1))
    blank = jnp.zeros((chan, chan), BF16)

    def forward(ref):
        base = None
        for off in range(3):
            tall = jnp.concatenate([ref[9 * a + 3 * off + b] for a, b in TAPS], axis=0)
            piece = dot(tall, one_hot(el == er + off * chan))
            base = piece if base is None else base + piece
        return [base[t * chan : (t + 1) * chan] for t in range(9)]

    def backward(ref):
        pieces = []
        for a, b in TAPS:
            tall = jnp.concatenate(
                [ref[26 - (9 * a + 3 * off + b)] for off in range(3)] + [blank], axis=0
            )
            pieces.append(dot(eye, tall, NT))
        return pieces

    def place_weights(n, pieces):
        extra = 9 * pack
        turned = []
        for t, b0 in enumerate(pieces):
            b1, b2, b3 = (pltpu.roll(b0, i * chan, 1) for i in (1, 2, 3))
            turned.append((b0, b1, b2, b3))
            mid = jnp.where(quad >= 2, b2, 0.0).astype(BF16)
            a0, a1 = b0.astype(BF16), b1.astype(BF16)
            low = jnp.where(quad < 2, b3, 0.0).astype(BF16)
            high = jnp.where(quad == 3, b3, 0.0).astype(BF16)
            for h, blocks in enumerate(((low, a0, a1, mid), (a0, a1, mid, high))):
                for y, block in enumerate(blocks):
                    wcat[n, h, y * chan : (y + 1) * chan, t * pack : (t + 1) * pack] = block

        def gather(off, q):
            value = jnp.zeros((chan, pack), F32)
            for t in range(4 * q, min(4 * q + 4, 9)):
                value = jnp.where(quad == t % 4, turned[t][(t - off) % 4], value)
            return value.astype(BF16)

        for q in range(3):
            at = slice(extra + q * pack, extra + (q + 1) * pack)
            last = gather(2, q)
            wcat[n, 0, 3 * chan : 4 * chan, at] = last
            wcat[n, 1, 2 * chan : 3 * chan, at] = last
            wcat[n, 1, 3 * chan : 4 * chan, at] = gather(1, q)

    for n in range(4):
        at = slice(9 * pack, 12 * pack)
        wcat[n, 0, : 3 * chan, at] = jnp.zeros((3 * chan, 3 * pack), BF16)
        wcat[n, 1, : 2 * chan, at] = jnp.zeros((2 * chan, 3 * pack), BF16)

    def scatter_terms(j):
        def send(slot, to_gz, to_dp):
            dev = to_gz * dp_count + to_dp

            @pl.when(dev < owners)
            def _():
                pltpu.make_async_remote_copy(
                    src_ref=packed.at[j, dev],
                    dst_ref=arrived.at[j, slot],
                    send_sem=rs_send.at[j],
                    recv_sem=rs_recv.at[j],
                    device_id={"gz": to_gz, "dp": to_dp},
                    device_id_type=MESH,
                ).start()

        each_peer(send)

    def wait_for(ref, sem):
        pltpu.make_async_copy(ref, ref, sem).wait()

    def gather_terms(j):
        @pl.when(me < owners)
        def _():
            wait_for(arrived.at[j], rs_recv.at[j])
            total = jnp.sum(arrived[j].astype(F32), axis=0) + packed[j, me].astype(F32)
            full[j, me] = total.astype(BF16)

            def send(slot, to_gz, to_dp):
                pltpu.make_async_remote_copy(
                    src_ref=full.at[j, me],
                    dst_ref=full.at[j, me],
                    send_sem=ag_send.at[j],
                    recv_sem=ag_recv.at[j],
                    device_id={"gz": to_gz, "dp": to_dp},
                    device_id_type=MESH,
                ).start()

            each_peer(send)

    def finish_terms(j):
        @pl.when(me < owners)
        def _():
            wait_for(full.at[j, pl.ds(0, owners - 1)], ag_recv.at[j])
            wait_for(packed.at[j, pl.ds(0, owners - 1)], rs_send.at[j])
            wait_for(arrived.at[j], ag_send.at[j])

        @pl.when(me >= owners)
        def _():
            wait_for(full.at[j, pl.ds(0, owners)], ag_recv.at[j])
            wait_for(packed.at[j, pl.ds(0, owners)], rs_send.at[j])

        sums_ref[j] = full[j]

    pr, pc = iota((3 * chan, 8 * chan), 0), iota((3 * chan, 8 * chan), 1)
    choose = one_hot(pc == (2 - pr // chan) * 2 * chan + pr % chan)

    def terms(j, s, s_grad):
        def source(pairs, plane, rel):
            cells = []
            for m in pairs:
                y = 2 * m + rel
                for p in range(depth):
                    if 0 <= y < height:
                        cells.append(s[1, p + plane, y * chan : (y + 1) * chan])
                    else:
                        cells.append(jnp.zeros((chan, width), BF16))
            return lanes(cells)

        def grad(pairs, col):
            return lanes(
                [
                    s_grad[col, p + 1, 2 * m * chan : (2 * m + 2) * chan]
                    for m in pairs
                    for p in range(depth)
                ]
            )

        def product(pairs):
            streamed = [source(pairs, plane, rel) for plane in range(3) for rel in range(-1, 3)]
            held = [grad(pairs, col) for col in (0, 1, 2, 1)]
            return dot(jnp.concatenate(streamed, axis=0), jnp.concatenate(held, axis=0), NT)

        values = [product(range(height // 4)), product(range(height // 4, height // 2))]

        def block(at, i):
            cells = slice(i * pack, (i + 1) * pack)
            return values[0][at : at + chan, cells] * factor + values[1][at : at + chan, cells] * factor

        blocks = []
        for plane in range(3):
            for off in range(3):
                at = (plane * 4 + off) * chan
                blocks.append(
                    lanes(
                        [
                            block(at, i) + pltpu.roll(block(at + chan, i), 3 * chan, 1)
                            for i in range(2)
                        ]
                    ).astype(BF16)
                )
        blocks.append(jnp.zeros((3 * chan, 8 * chan), BF16))
        turned = dot(choose, jnp.concatenate(blocks, axis=0), NT)
        tail = turned[:, 2 * pack :]
        tail = (
            tail[:chan]
            + pltpu.roll(tail[chan : 2 * chan], chan, 1)
            + pltpu.roll(tail[2 * chan :], 2 * chan, 1)
        )
        tiles = packed.shape[2]
        sources = [
            turned[8 * i : 8 * i + 8, g * pack : (g + 1) * pack]
            for i in range(3 * chan // 8)
            for g in range(2)
        ] + [tail[8 * i : 8 * i + 8] for i in range(chan // 8)]
        for t, tile in enumerate(sources):
            packed[j, t // tiles, t % tiles] = tile.astype(BF16)

    if owners * packed.shape[2] > 28:
        packed[...] = jnp.zeros_like(packed)

    def first_layer(planes):
        for h in range(2):
            at = pl.ds(h * part_rows, part_rows)
            for p, pre in zip(planes, conv(0, s_in, planes, h)):
                sig = sigmoid(pre)
                slope[p, at] = sig * (1.0 + pre * (1.0 - sig))
                put(s_hid, p + 1, h, pre * sig)

    def second_layer(planes):
        cots = load(cot_ref, planes)
        for h in range(2):
            for p, pre, cot in zip(planes, conv(1, s_hid, planes, h), cots):
                sig = sigmoid(pre)
                cot = cot[h * part_rows : (h + 1) * part_rows]
                put(s_g2, p + 1, h, cot * (sig * (1.0 + pre * (1.0 - sig))))

    def second_back(planes):
        for h in range(2):
            at = pl.ds(h * part_rows, part_rows)
            for p, value in zip(planes, conv(2, s_g2, planes, h)):
                put(s_g1, p + 1, h, value * slope[p, at])

    def first_back(planes):
        value = jnp.concatenate(
            [lanes(conv(3, s_g1, planes, h)).astype(BF16) for h in range(2)], axis=0
        )
        for p, part in zip(planes, split(dot(perm[1], value), planes)):
            out_ref[:, p] = part.reshape(chan, height, width).astype(BF16)

    loads[0].wait()
    place_weights(0, forward(w1_ref))
    loads[1].wait()
    for planes in groups:
        for p, value in zip(planes, load(x_ref, planes)):
            for h in range(2):
                put(s_in, p + 1, h, value[h * part_rows : (h + 1) * part_rows])
    for planes in groups[1:]:
        first_layer(planes)
    pl.semaphore_wait(barrier, count - 1)
    send_halo(0)
    for copy in loads[2:]:
        copy.wait()
    place_weights(1, forward(w2_ref))
    place_weights(2, backward(w2_ref))
    take_halo(0)
    first_layer(groups[0])
    send_halo(1)
    for planes in groups[1:]:
        second_layer(planes)
    place_weights(3, backward(w1_ref))
    take_halo(1)
    second_layer(groups[0])
    send_halo(2)
    terms(1, s_hid, s_g2)
    scatter_terms(1)
    take_halo(2)
    for i, planes in enumerate(groups):
        second_back(planes)
        if i == 0:
            send_halo(3)
    terms(0, s_in, s_g1)
    scatter_terms(0)
    take_halo(3)
    for planes in groups:
        first_back(planes)
    gather_terms(1)
    gather_terms(0)
    finish_terms(1)
    finish_terms(0)

    for n in range(4):

        @pl.when(gz < gz_count - 1)
        def _():
            up_copy(n).wait_send()

        @pl.when(gz > 0)
        def _():
            down_copy(n).wait_send()


def unpack(out_ref, sums_ref, out_hbm, g1_hbm, g2_hbm, grads_ref, sems):
    chan = out_ref.shape[0]
    store_out = pltpu.make_async_copy(out_ref, out_hbm, sems.at[2])
    store_out.start()
    store = [
        pltpu.make_async_copy(grads_ref.at[j], g, sems.at[j]) for j, g in enumerate((g1_hbm, g2_hbm))
    ]
    groups = chan // 8
    for j in range(2):
        for kx in range(3):
            for o in range(groups):
                at = slice(8 * o, 8 * o + 8)
                for g in range(2):
                    tile = sums_ref[j, (kx * groups + o) * 2 + g].astype(F32)
                    for i in range(4):
                        t = (4 * g + i) * 3 + kx
                        grads_ref[j, t, at] = tile[:, i * chan : (i + 1) * chan]
        for o in range(groups):
            tile = sums_ref[j, 6 * groups + o].astype(F32)
            for kx in range(3):
                grads_ref[j, 24 + kx, 8 * o : 8 * o + 8] = tile[:, kx * chan : (kx + 1) * chan]
        store[j].start()
    for move in store:
        move.wait()
    store_out.wait()


def solution(mesh):
    gz_count, dp_count = mesh.shape["gz"], mesh.shape["dp"]
    count = gz_count * dp_count

    def local(inputs, kernel_one, kernel_two, cotangent):
        _, chan, depth, height, width = inputs.shape
        rows = chan * height
        cells = dp_count * gz_count * depth * height * width
        tiles = -(-28 // count)
        owners = -(-28 // tiles)
        taps = lambda k: k.transpose(2, 3, 4, 0, 1).reshape(27, chan, chan)
        slab = pltpu.VMEM((3, depth + 2, rows, width), BF16)
        vmem = pl.BlockSpec(memory_space=pltpu.VMEM)
        anywhere = pl.BlockSpec(memory_space=pl.ANY)
        out, sums = pl.pallas_call(
            functools.partial(kernel, (gz_count, dp_count, owners), 1.0 / math.sqrt(cells)),
            out_shape=(
                pltpu.VMEM((chan, depth, height, width), BF16),
                pltpu.VMEM((2, owners, tiles, 8, 128), BF16),
            ),
            in_specs=[anywhere] * 4,
            out_specs=(vmem, vmem),
            scratch_shapes=[
                pltpu.VMEM((chan, depth, height, width), BF16),
                pltpu.VMEM((27, chan, chan), BF16),
                pltpu.VMEM((27, chan, chan), BF16),
                pltpu.VMEM((chan, depth, height, width), BF16),
                slab,
                slab,
                slab,
                slab,
                pltpu.VMEM((4, 2, rows // 2, 12 * 4 * chan), BF16),
                pltpu.VMEM((depth, rows, width), F32),
                pltpu.VMEM((2, rows, rows), BF16),
                pltpu.VMEM((2, owners, tiles, 8, 128), BF16),
                pltpu.VMEM((2, count - 1, tiles, 8, 128), BF16),
                pltpu.VMEM((2, owners, tiles, 8, 128), BF16),
                pltpu.SemaphoreType.DMA((4, 2)),
                pltpu.SemaphoreType.DMA((4, 2)),
                pltpu.SemaphoreType.DMA((2,)),
                pltpu.SemaphoreType.DMA((2,)),
                pltpu.SemaphoreType.DMA((2,)),
                pltpu.SemaphoreType.DMA((2,)),
                pltpu.SemaphoreType.DMA((4,)),
            ],
            compiler_params=pltpu.CompilerParams(collective_id=0, has_side_effects=True),
        )(inputs[0], taps(kernel_one), taps(kernel_two), cotangent[0])
        sums = sums.reshape(2, owners * tiles, 8, 128)
        out, sums = (pltpu.with_memory_space_constraint(v, pltpu.VMEM) for v in (out, sums))
        out, g1, g2 = pl.pallas_call(
            unpack,
            out_shape=(
                jax.ShapeDtypeStruct((chan, depth, height, width), BF16),
                jax.ShapeDtypeStruct((27, chan, chan), F32),
                jax.ShapeDtypeStruct((27, chan, chan), F32),
            ),
            in_specs=[vmem] * 2,
            out_specs=(anywhere,) * 3,
            scratch_shapes=[
                pltpu.VMEM((2, 27, chan, chan), F32),
                pltpu.SemaphoreType.DMA((3,)),
            ],
        )(out, sums)
        back = lambda g: g.reshape(3, 3, 3, chan, chan).transpose(3, 4, 0, 1, 2)
        return out[None], back(g1), back(g2)

    return jax.shard_map(
        local,
        mesh=mesh,
        in_specs=(P("dp", None, "gz", None, None), P(), P(), P("dp", None, "gz", None, None)),
        out_specs=(P("dp", None, "gz", None, None), P(), P()),
        check_vma=False,
    )
```

```python
import functools
import math

import jax
import jax.numpy as jnp
from jax import lax
from jax.experimental import pallas as pl
from jax.experimental.pallas import tpu as pltpu
from jax.sharding import PartitionSpec as P

MESH = pl.DeviceIdType.MESH
F32 = jnp.float32
BF16 = jnp.bfloat16
TAPS = [(plane, col) for plane in range(3) for col in range(3)]
NN = (((1,), (0,)), ((), ()))
NT = (((1,), (1,)), ((), ()))
UNROLL_UP_TO = 64


def dot(a, b, dims=NN):
    return lax.dot_general(a, b, dims, preferred_element_type=F32)


def iota(shape, dim):
    return lax.broadcasted_iota(jnp.int32, shape, dim)


def one_hot(mask):
    return jnp.where(mask, 1.0, 0.0).astype(BF16)


def sigmoid(v):
    return 0.5 * jnp.tanh(0.5 * v) + 0.5


def kernel(
    sizes,
    factor,
    x_hbm,
    w1_hbm,
    w2_hbm,
    cot_hbm,
    out_ref,
    sums_ref,
    x_ref,
    w1_ref,
    w2_ref,
    cot_ref,
    s_in,
    s_hid,
    s_g2,
    s_g1,
    wcat,
    slope,
    perm,
    sums_acc,
    packed,
    arrived,
    full,
    halo_send,
    halo_recv,
    rs_send,
    rs_recv,
    ag_send,
    ag_recv,
    load_sem,
):
    gz_count, dp_count, owners, own = sizes
    chan, depth, height, width = x_ref.shape
    rows = chan * height
    half = height // 2
    part_rows = half * chan
    pack = 4 * chan
    count = gz_count * dp_count
    gz = lax.axis_index("gz")
    dp = lax.axis_index("dp")
    me = gz * dp_count + dp

    loads = [
        pltpu.make_async_copy(src, dst, load_sem.at[i])
        for i, (src, dst) in enumerate(
            ((w1_hbm, w1_ref), (x_hbm, x_ref), (w2_hbm, w2_ref), (cot_hbm, cot_ref))
        )
    ]
    for copy in loads:
        copy.start()

    barrier = pltpu.get_barrier_semaphore()
    outer = 4 if dp_count % 4 == 0 else 1
    inner_count = dp_count // outer
    dp_out, dp_in = dp // inner_count, lax.rem(dp, inner_count)
    offsets = [
        (g, a, b)
        for a in sorted(range(outer), key=lambda a: -min(a, outer - a))
        for b in reversed(range(inner_count))
        for g in range(gz_count)
        if g or a or b
    ]

    def each_peer(act):
        if count <= UNROLL_UP_TO:
            to_gz = [lax.rem(gz + g, gz_count) for g in range(gz_count)]
            to_out = [lax.rem(dp_out + a, outer) * inner_count for a in range(outer)]
            to_in = [lax.rem(dp_in + b, inner_count) for b in range(inner_count)]
            for slot, (g, a, b) in enumerate(offsets):
                act(slot, to_gz[g], to_out[a] + to_in[b])
        else:

            def step(k, carry):
                dev = lax.rem(me + k, count)
                act(k - 1, dev // dp_count, lax.rem(dev, dp_count))
                return carry

            lax.fori_loop(1, count, step, 0)

    own_gz, own_low, own_count = own

    def rank_of(at_dp):
        return at_dp - own_low

    def is_owner(at_gz, at_dp):
        inside = (at_dp >= own_low) & (at_dp < own_low + min(own_count, owners))
        return inside & (at_gz == own_gz)

    rank, owner = rank_of(dp), is_owner(gz, dp)

    def greet(slot, to_gz, to_dp):
        pl.semaphore_signal(
            barrier, inc=1, device_id={"gz": to_gz, "dp": to_dp}, device_id_type=MESH
        )

    each_peer(greet)

    slabs = (s_in, s_hid, s_g2, s_g1)

    @pl.when(gz == 0)
    def _():
        for s in slabs:
            s[:, 0] = jnp.zeros((3, rows, width), BF16)

    @pl.when(gz == gz_count - 1)
    def _():
        for s in slabs:
            s[:, depth + 1] = jnp.zeros((3, rows, width), BF16)

    r, l = iota((rows, rows), 0), iota((rows, rows), 1)
    perm[0] = one_hot((r // chan == l % height) & (r % chan == l // height))
    perm[1] = one_hot((r // height == l % chan) & (r % height == l // chan))

    lane_of = iota((part_rows, width), 1)
    not_first, not_last = lane_of != 0, lane_of != width - 1

    def put(s, p, h, value):
        at = pl.ds(h * part_rows, part_rows)
        s[1, p, at] = value.astype(BF16)
        s[0, p, at] = jnp.where(not_first, pltpu.roll(value, 1, 1), 0.0).astype(BF16)
        s[2, p, at] = jnp.where(not_last, pltpu.roll(value, width - 1, 1), 0.0).astype(BF16)

    def up_copy(n):
        return pltpu.make_async_remote_copy(
            src_ref=slabs[n].at[:, depth],
            dst_ref=slabs[n].at[:, 0],
            send_sem=halo_send.at[n, 0],
            recv_sem=halo_recv.at[n, 0],
            device_id={"gz": gz + 1, "dp": dp},
            device_id_type=MESH,
        )

    def down_copy(n):
        return pltpu.make_async_remote_copy(
            src_ref=slabs[n].at[:, 1],
            dst_ref=slabs[n].at[:, depth + 1],
            send_sem=halo_send.at[n, 1],
            recv_sem=halo_recv.at[n, 1],
            device_id={"gz": gz - 1, "dp": dp},
            device_id_type=MESH,
        )

    def send_halo(n):
        @pl.when(gz < gz_count - 1)
        def _():
            up_copy(n).start()

        @pl.when(gz > 0)
        def _():
            down_copy(n).start()

    def take_halo(n):
        @pl.when(gz > 0)
        def _():
            up_copy(n).wait_recv()

        @pl.when(gz < gz_count - 1)
        def _():
            down_copy(n).wait_recv()

    def raw(ref, p):
        return ref[:, p].astype(F32).reshape(rows, width).astype(BF16)

    edges = sorted({0, depth - 1})
    inner = [p for p in range(depth) if p not in edges]
    groups = [edges] + [inner[i : i + 2] for i in range(0, len(inner), 2)]

    def lanes(parts):
        return parts[0] if len(parts) == 1 else jnp.concatenate(parts, axis=1)

    def split(value, planes):
        return [value[:, i * width : (i + 1) * width] for i in range(len(planes))]

    def load(ref, planes):
        return split(dot(perm[0], lanes([raw(ref, p) for p in planes])), planes)

    def conv(n, s, planes, h):
        first = h * (half - 1) * chan
        span = lambda at, size: [
            lanes([s[col, p + plane, at : at + size] for p in planes]) for plane, col in TAPS
        ]
        window = jnp.concatenate(
            span(first, part_rows) + span(first + part_rows, chan), axis=0
        )
        return split(dot(wcat[n, h, :, : 9 * (part_rows + chan)], window), planes)

    lane32 = iota((chan, pack), 1)
    quad = lane32 // chan
    er, el = iota((chan, pack), 0), lane32
    eye = one_hot(iota((chan, chan), 0) == iota((chan, chan), 1))
    blank = jnp.zeros((chan, chan), BF16)

    def forward(ref):
        base = None
        for off in range(3):
            tall = jnp.concatenate([ref[9 * a + 3 * off + b] for a, b in TAPS], axis=0)
            piece = dot(tall, one_hot(el == er + off * chan))
            base = piece if base is None else base + piece
        return [base[t * chan : (t + 1) * chan] for t in range(9)]

    def backward(ref):
        pieces = []
        for a, b in TAPS:
            tall = jnp.concatenate(
                [ref[26 - (9 * a + 3 * off + b)] for off in range(3)] + [blank], axis=0
            )
            pieces.append(dot(eye, tall, NT))
        return pieces

    def place_weights(n, pieces):
        extra = 9 * pack
        turned = []
        for t, b0 in enumerate(pieces):
            b1, b2, b3 = (pltpu.roll(b0, i * chan, 1) for i in (1, 2, 3))
            turned.append((b0, b1, b2, b3))
            mid = jnp.where(quad >= 2, b2, 0.0).astype(BF16)
            a0, a1 = b0.astype(BF16), b1.astype(BF16)
            low = jnp.where(quad < 2, b3, 0.0).astype(BF16)
            high = jnp.where(quad == 3, b3, 0.0).astype(BF16)
            for h, blocks in enumerate(((low, a0, a1, mid), (a0, a1, mid, high))):
                for y, block in enumerate(blocks):
                    wcat[n, h, y * chan : (y + 1) * chan, t * pack : (t + 1) * pack] = block

        def gather(off, q):
            value = jnp.zeros((chan, pack), F32)
            for t in range(4 * q, min(4 * q + 4, 9)):
                value = jnp.where(quad == t % 4, turned[t][(t - off) % 4], value)
            return value.astype(BF16)

        for q in range(3):
            at = slice(extra + q * pack, extra + (q + 1) * pack)
            last = gather(2, q)
            wcat[n, 0, 3 * chan : 4 * chan, at] = last
            wcat[n, 1, 2 * chan : 3 * chan, at] = last
            wcat[n, 1, 3 * chan : 4 * chan, at] = gather(1, q)

    for n in range(4):
        at = slice(9 * pack, 12 * pack)
        wcat[n, 0, : 3 * chan, at] = jnp.zeros((3 * chan, 3 * pack), BF16)
        wcat[n, 1, : 2 * chan, at] = jnp.zeros((2 * chan, 3 * pack), BF16)

    def scatter_terms(j):
        def send(slot, to_gz, to_dp):
            @pl.when(is_owner(to_gz, to_dp))
            def _():
                pltpu.make_async_remote_copy(
                    src_ref=packed.at[j, rank_of(to_dp)],
                    dst_ref=arrived.at[j, slot],
                    send_sem=rs_send.at[j],
                    recv_sem=rs_recv.at[j],
                    device_id={"gz": to_gz, "dp": to_dp},
                    device_id_type=MESH,
                ).start()

        each_peer(send)

    def wait_for(ref, sem):
        pltpu.make_async_copy(ref, ref, sem).wait()

    def gather_terms(j):
        @pl.when(owner)
        def _():
            wait_for(arrived.at[j], rs_recv.at[j])
            total = jnp.sum(arrived[j].astype(F32), axis=0) + packed[j, rank].astype(F32)
            full[j, rank] = total.astype(BF16)

            def send(slot, to_gz, to_dp):
                pltpu.make_async_remote_copy(
                    src_ref=full.at[j, rank],
                    dst_ref=full.at[j, rank],
                    send_sem=ag_send.at[j],
                    recv_sem=ag_recv.at[j],
                    device_id={"gz": to_gz, "dp": to_dp},
                    device_id_type=MESH,
                ).start()

            each_peer(send)

    def finish_terms(j):
        @pl.when(owner)
        def _():
            wait_for(full.at[j, pl.ds(0, owners - 1)], ag_recv.at[j])
            wait_for(packed.at[j, pl.ds(0, owners - 1)], rs_send.at[j])
            wait_for(arrived.at[j], ag_send.at[j])

        @pl.when(jnp.logical_not(owner))
        def _():
            wait_for(full.at[j, pl.ds(0, owners)], ag_recv.at[j])
            wait_for(packed.at[j, pl.ds(0, owners)], rs_send.at[j])

        sums_ref[j] = full[j]

    pr, pc = iota((3 * chan, 8 * chan), 0), iota((3 * chan, 8 * chan), 1)
    choose = one_hot(pc == (2 - pr // chan) * 2 * chan + pr % chan)

    halves = [range(height // 4), range(height // 4, height // 2)]

    def products(s, s_grad, planes):
        def source(pairs, plane, rel):
            cells = []
            for m in pairs:
                y = 2 * m + rel
                for p in planes:
                    if 0 <= y < height:
                        cells.append(s[1, p + plane, y * chan : (y + 1) * chan])
                    else:
                        cells.append(jnp.zeros((chan, width), BF16))
            return lanes(cells)

        def grad(pairs, col):
            return lanes(
                [
                    s_grad[col, p + 1, 2 * m * chan : (2 * m + 2) * chan]
                    for m in pairs
                    for p in planes
                ]
            )

        values = []
        for pairs in halves:
            streamed = [source(pairs, plane, rel) for plane in range(3) for rel in range(-1, 3)]
            held = [grad(pairs, col) for col in (0, 1, 2, 1)]
            values.append(
                dot(jnp.concatenate(streamed, axis=0), jnp.concatenate(held, axis=0), NT)
            )
        return values

    def add_terms(j, s, s_grad, planes, first=False):
        one, two = products(s, s_grad, planes)
        value = one * factor + two * factor
        sums_acc[j] = value if first else sums_acc[j] + value

    def end_terms(j, s, s_grad, planes):
        one, two = products(s, s_grad, planes)

        def block(at, i):
            cells = slice(i * pack, (i + 1) * pack)
            rest = one[at : at + chan, cells] * factor + two[at : at + chan, cells] * factor
            return sums_acc[j, at : at + chan, cells] + rest

        blocks = []
        for plane in range(3):
            for off in range(3):
                at = (plane * 4 + off) * chan
                blocks.append(
                    lanes(
                        [
                            block(at, i) + pltpu.roll(block(at + chan, i), 3 * chan, 1)
                            for i in range(2)
                        ]
                    ).astype(BF16)
                )
        blocks.append(jnp.zeros((3 * chan, 8 * chan), BF16))
        turned = dot(choose, jnp.concatenate(blocks, axis=0), NT)
        tail = turned[:, 2 * pack :]
        tail = (
            tail[:chan]
            + pltpu.roll(tail[chan : 2 * chan], chan, 1)
            + pltpu.roll(tail[2 * chan :], 2 * chan, 1)
        )
        tiles = packed.shape[2]
        sources = [
            turned[8 * i : 8 * i + 8, g * pack : (g + 1) * pack]
            for i in range(3 * chan // 8)
            for g in range(2)
        ] + [tail[8 * i : 8 * i + 8] for i in range(chan // 8)]
        for t, tile in enumerate(sources):
            packed[j, t // tiles, t % tiles] = tile.astype(BF16)

    if owners * packed.shape[2] > 28:
        packed[...] = jnp.zeros_like(packed)

    def first_layer(planes):
        for h in range(2):
            at = pl.ds(h * part_rows, part_rows)
            for p, pre in zip(planes, conv(0, s_in, planes, h)):
                sig = sigmoid(pre)
                slope[p, at] = sig * (1.0 + pre * (1.0 - sig))
                put(s_hid, p + 1, h, pre * sig)

    def second_layer(planes):
        cots = load(cot_ref, planes)
        for h in range(2):
            for p, pre, cot in zip(planes, conv(1, s_hid, planes, h), cots):
                sig = sigmoid(pre)
                cot = cot[h * part_rows : (h + 1) * part_rows]
                put(s_g2, p + 1, h, cot * (sig * (1.0 + pre * (1.0 - sig))))

    def second_back(planes):
        for h in range(2):
            at = pl.ds(h * part_rows, part_rows)
            for p, value in zip(planes, conv(2, s_g2, planes, h)):
                put(s_g1, p + 1, h, value * slope[p, at])

    def first_back(planes):
        value = jnp.concatenate(
            [lanes(conv(3, s_g1, planes, h)).astype(BF16) for h in range(2)], axis=0
        )
        for p, part in zip(planes, split(dot(perm[1], value), planes)):
            out_ref[:, p] = part.reshape(chan, height, width).astype(BF16)

    ring = lambda k: sorted({k, depth - 1 - k})
    core = [p for p in range(2, depth - 2)]
    core = [core[i : i + 2] for i in range(0, len(core), 2)]
    loads[0].wait()
    place_weights(0, forward(w1_ref))
    loads[1].wait()
    for planes in groups:
        for p, value in zip(planes, load(x_ref, planes)):
            for h in range(2):
                put(s_in, p + 1, h, value[h * part_rows : (h + 1) * part_rows])
    for copy in loads[2:]:
        copy.wait()
    for i, planes in enumerate(groups[1:]):
        first_layer(planes)
        if i == 0:
            place_weights(1, forward(w2_ref))
    pl.semaphore_wait(barrier, count - 1)
    send_halo(0)
    for i, planes in enumerate(core):
        second_layer(planes)
        if i == 0:
            place_weights(2, backward(w2_ref))
    add_terms(1, s_hid, s_g2, core[0], True)
    take_halo(0)
    first_layer(ring(0))
    send_halo(1)
    for planes in core[1:]:
        add_terms(1, s_hid, s_g2, planes)
    second_layer(ring(1))
    for planes in core:
        second_back(planes)
    take_halo(1)
    second_layer(ring(0))
    send_halo(2)
    for i, planes in enumerate(core):
        add_terms(0, s_in, s_g1, planes, i == 0)
    second_back(ring(1))
    end_terms(1, s_hid, s_g2, ring(0) + ring(1))
    scatter_terms(1)
    take_halo(2)
    second_back(ring(0))
    send_halo(3)
    end_terms(0, s_in, s_g1, ring(0) + ring(1))
    scatter_terms(0)
    place_weights(3, backward(w1_ref))
    for planes in groups[1:]:
        first_back(planes)
    take_halo(3)
    first_back(ring(0))
    gather_terms(1)
    gather_terms(0)
    finish_terms(1)
    finish_terms(0)

    for n in range(4):

        @pl.when(gz < gz_count - 1)
        def _():
            up_copy(n).wait_send()

        @pl.when(gz > 0)
        def _():
            down_copy(n).wait_send()


def unpack(out_ref, sums_ref, out_hbm, g1_hbm, g2_hbm, grads_ref, sems):
    chan = out_ref.shape[0]
    store_out = pltpu.make_async_copy(out_ref, out_hbm, sems.at[2])
    store_out.start()
    store = [
        pltpu.make_async_copy(grads_ref.at[j], g, sems.at[j]) for j, g in enumerate((g1_hbm, g2_hbm))
    ]
    groups = chan // 8
    for j in range(2):
        for kx in range(3):
            for o in range(groups):
                at = slice(8 * o, 8 * o + 8)
                for g in range(2):
                    tile = sums_ref[j, (kx * groups + o) * 2 + g].astype(F32)
                    for i in range(4):
                        t = (4 * g + i) * 3 + kx
                        grads_ref[j, t, at] = tile[:, i * chan : (i + 1) * chan]
        for o in range(groups):
            tile = sums_ref[j, 6 * groups + o].astype(F32)
            for kx in range(3):
                grads_ref[j, 24 + kx, 8 * o : 8 * o + 8] = tile[:, kx * chan : (kx + 1) * chan]
        store[j].start()
    for move in store:
        move.wait()
    store_out.wait()


def solution(mesh):
    gz_count, dp_count = mesh.shape["gz"], mesh.shape["dp"]
    count = gz_count * dp_count

    def local(inputs, kernel_one, kernel_two, cotangent):
        _, chan, depth, height, width = inputs.shape
        rows = chan * height
        cells = dp_count * gz_count * depth * height * width
        own_count = dp_count // 2 if dp_count % 4 == 0 else dp_count
        own_low = (dp_count - own_count) // 2
        tiles = -(-28 // own_count)
        owners = -(-28 // tiles)
        taps = lambda k: k.transpose(2, 3, 4, 0, 1).reshape(27, chan, chan)
        slab = pltpu.VMEM((3, depth + 2, rows, width), BF16)
        vmem = pl.BlockSpec(memory_space=pltpu.VMEM)
        anywhere = pl.BlockSpec(memory_space=pl.ANY)
        out, sums = pl.pallas_call(
            functools.partial(kernel, (gz_count, dp_count, owners, (gz_count - 1, own_low, own_count)), 1.0 / math.sqrt(cells)),
            out_shape=(
                pltpu.VMEM((chan, depth, height, width), BF16),
                pltpu.VMEM((2, owners, tiles, 8, 128), BF16),
            ),
            in_specs=[anywhere] * 4,
            out_specs=(vmem, vmem),
            scratch_shapes=[
                pltpu.VMEM((chan, depth, height, width), BF16),
                pltpu.VMEM((27, chan, chan), BF16),
                pltpu.VMEM((27, chan, chan), BF16),
                pltpu.VMEM((chan, depth, height, width), BF16),
                slab,
                slab,
                slab,
                slab,
                pltpu.VMEM((4, 2, rows // 2, 12 * 4 * chan), BF16),
                pltpu.VMEM((depth, rows, width), F32),
                pltpu.VMEM((2, rows, rows), BF16),
                pltpu.VMEM((2, 12 * chan, 8 * chan), F32),
                pltpu.VMEM((2, owners, tiles, 8, 128), BF16),
                pltpu.VMEM((2, count - 1, tiles, 8, 128), BF16),
                pltpu.VMEM((2, owners, tiles, 8, 128), BF16),
                pltpu.SemaphoreType.DMA((4, 2)),
                pltpu.SemaphoreType.DMA((4, 2)),
                pltpu.SemaphoreType.DMA((2,)),
                pltpu.SemaphoreType.DMA((2,)),
                pltpu.SemaphoreType.DMA((2,)),
                pltpu.SemaphoreType.DMA((2,)),
                pltpu.SemaphoreType.DMA((4,)),
            ],
            compiler_params=pltpu.CompilerParams(collective_id=0, has_side_effects=True),
        )(inputs[0], taps(kernel_one), taps(kernel_two), cotangent[0])
        sums = sums.reshape(2, owners * tiles, 8, 128)
        out, sums = (pltpu.with_memory_space_constraint(v, pltpu.VMEM) for v in (out, sums))
        out, g1, g2 = pl.pallas_call(
            unpack,
            out_shape=(
                jax.ShapeDtypeStruct((chan, depth, height, width), BF16),
                jax.ShapeDtypeStruct((27, chan, chan), F32),
                jax.ShapeDtypeStruct((27, chan, chan), F32),
            ),
            in_specs=[vmem] * 2,
            out_specs=(anywhere,) * 3,
            scratch_shapes=[
                pltpu.VMEM((2, 27, chan, chan), F32),
                pltpu.SemaphoreType.DMA((3,)),
            ],
        )(out, sums)
        back = lambda g: g.reshape(3, 3, 3, chan, chan).transpose(3, 4, 0, 1, 2)
        return out[None], back(g1), back(g2)

    return jax.shard_map(
        local,
        mesh=mesh,
        in_specs=(P("dp", None, "gz", None, None), P(), P(), P("dp", None, "gz", None, None)),
        out_specs=(P("dp", None, "gz", None, None), P(), P()),
        check_vma=False,
    )
```

```python
import functools
import math

import jax
import jax.numpy as jnp
from jax import lax
from jax.experimental import pallas as pl
from jax.experimental.pallas import tpu as pltpu
from jax.sharding import PartitionSpec as P

MESH = pl.DeviceIdType.MESH
F32 = jnp.float32
BF16 = jnp.bfloat16
TAPS = [(plane, col) for plane in range(3) for col in range(3)]
NN = (((1,), (0,)), ((), ()))
NT = (((1,), (1,)), ((), ()))
UNROLL_UP_TO = 64


def dot(a, b, dims=NN):
    return lax.dot_general(a, b, dims, preferred_element_type=F32)


def iota(shape, dim):
    return lax.broadcasted_iota(jnp.int32, shape, dim)


def one_hot(mask):
    return jnp.where(mask, 1.0, 0.0).astype(BF16)


def sigmoid(v):
    return 0.5 * jnp.tanh(0.5 * v) + 0.5


def kernel(
    sizes,
    factor,
    x_hbm,
    w1_hbm,
    w2_hbm,
    cot_hbm,
    out_ref,
    grads_ref,
    x_ref,
    w1_ref,
    w2_ref,
    cot_ref,
    s_in,
    s_hid,
    s_g2,
    s_g1,
    wcat,
    slope,
    perm,
    sums_acc,
    packed,
    arrived,
    full,
    halo_send,
    halo_recv,
    rs_send,
    rs_recv,
    ag_send,
    ag_recv,
    load_sem,
):
    gz_count, dp_count, owners, own = sizes
    chan, depth, height, width = x_ref.shape
    rows = chan * height
    half = height // 2
    part_rows = half * chan
    pack = 4 * chan
    count = gz_count * dp_count
    gz = lax.axis_index("gz")
    dp = lax.axis_index("dp")
    me = gz * dp_count + dp

    loads = [
        pltpu.make_async_copy(src, dst, load_sem.at[i])
        for i, (src, dst) in enumerate(
            ((x_hbm, x_ref), (w1_hbm, w1_ref), (w2_hbm, w2_ref), (cot_hbm, cot_ref))
        )
    ]
    for copy in loads:
        copy.start()

    barrier = pltpu.get_barrier_semaphore()
    outer = 4 if dp_count % 4 == 0 else 1
    inner_count = dp_count // outer
    dp_out, dp_in = dp // inner_count, lax.rem(dp, inner_count)
    far_first = sorted(range(outer), key=lambda a: -min(a, outer - a))
    offsets = [
        (g, a, b)
        for a in far_first
        for b in reversed(range(inner_count))
        for g in range(gz_count)
        if g or a or b
    ]

    def each_peer(act):
        if count <= UNROLL_UP_TO:
            to_gz = [lax.rem(gz + g, gz_count) for g in range(gz_count)]
            to_out = [lax.rem(dp_out + a, outer) * inner_count for a in range(outer)]
            to_in = [lax.rem(dp_in + b, inner_count) for b in range(inner_count)]
            for slot, (g, a, b) in enumerate(offsets):
                act(slot, to_gz[g], to_out[a] + to_in[b])
        else:

            def step(k, carry):
                dev = lax.rem(me + k, count)
                act(k - 1, dev // dp_count, lax.rem(dev, dp_count))
                return carry

            lax.fori_loop(1, count, step, 0)

    own_gz, own_low = own
    rank = dp - own_low
    owner = (gz == own_gz) & (rank >= 0) & (rank < owners)


    def greet(slot, to_gz, to_dp):
        pl.semaphore_signal(
            barrier, inc=1, device_id={"gz": to_gz, "dp": to_dp}, device_id_type=MESH
        )

    each_peer(greet)

    slabs = (s_in, s_hid, s_g2, s_g1)

    @pl.when(gz == 0)
    def _():
        for s in slabs:
            s[:, 0] = jnp.zeros((3, rows, width), BF16)

    @pl.when(gz == gz_count - 1)
    def _():
        for s in slabs:
            s[:, depth + 1] = jnp.zeros((3, rows, width), BF16)

    r, l = iota((rows, rows), 0), iota((rows, rows), 1)
    perm[0] = one_hot((r // chan == l % height) & (r % chan == l // height))
    perm[1] = one_hot((r // height == l % chan) & (r % height == l // chan))

    lane_of = iota((part_rows, width), 1)
    not_first, not_last = one_hot(lane_of != 0), one_hot(lane_of != width - 1)

    def put(s, p, h, value):
        at = pl.ds(h * part_rows, part_rows)
        value = value.astype(BF16)
        s[1, p, at] = value
        s[0, p, at] = not_first * pltpu.roll(value, 1, 1)
        s[2, p, at] = not_last * pltpu.roll(value, width - 1, 1)

    def up_copy(n):
        return pltpu.make_async_remote_copy(
            src_ref=slabs[n].at[:, depth],
            dst_ref=slabs[n].at[:, 0],
            send_sem=halo_send.at[n, 0],
            recv_sem=halo_recv.at[n, 0],
            device_id={"gz": gz + 1, "dp": dp},
            device_id_type=MESH,
        )

    def down_copy(n):
        return pltpu.make_async_remote_copy(
            src_ref=slabs[n].at[:, 1],
            dst_ref=slabs[n].at[:, depth + 1],
            send_sem=halo_send.at[n, 1],
            recv_sem=halo_recv.at[n, 1],
            device_id={"gz": gz - 1, "dp": dp},
            device_id_type=MESH,
        )

    def send_halo(n):
        @pl.when(gz < gz_count - 1)
        def _():
            up_copy(n).start()

        @pl.when(gz > 0)
        def _():
            down_copy(n).start()

    def take_halo(n):
        @pl.when(gz > 0)
        def _():
            up_copy(n).wait_recv()

        @pl.when(gz < gz_count - 1)
        def _():
            down_copy(n).wait_recv()

    def raw(ref, p):
        return ref[:, p].astype(F32).reshape(rows, width).astype(BF16)

    edges = sorted({0, depth - 1})
    inner = [p for p in range(depth) if p not in edges]
    groups = [edges] + [inner[i : i + 2] for i in range(0, len(inner), 2)]

    def lanes(parts):
        return parts[0] if len(parts) == 1 else jnp.concatenate(parts, axis=1)

    def split(value, planes):
        return [value[:, i * width : (i + 1) * width] for i in range(len(planes))]

    def load(ref, planes):
        return split(dot(perm[0], lanes([raw(ref, p) for p in planes])), planes)

    def conv(n, s, planes, h):
        first = h * (half - 1) * chan
        span = lambda at, size: [
            lanes([s[col, p + plane, at : at + size] for p in planes]) for plane, col in TAPS
        ]
        window = jnp.concatenate(
            span(first, part_rows) + span(first + part_rows, chan), axis=0
        )
        return split(dot(wcat[n, h, :, : 9 * (part_rows + chan)], window), planes)

    lane32 = iota((chan, pack), 1)
    quad = lane32 // chan
    er, el = iota((chan, pack), 0), lane32
    eye = one_hot(iota((chan, chan), 0) == iota((chan, chan), 1))
    blank = jnp.zeros((chan, chan), BF16)

    def forward(ref):
        base = None
        for off in range(3):
            tall = jnp.concatenate([ref[9 * a + 3 * off + b] for a, b in TAPS], axis=0)
            piece = dot(tall, one_hot(el == er + off * chan))
            base = piece if base is None else base + piece
        return [base[t * chan : (t + 1) * chan] for t in range(9)]

    def backward(ref):
        pieces = []
        for a, b in TAPS:
            tall = jnp.concatenate(
                [ref[26 - (9 * a + 3 * off + b)] for off in range(3)] + [blank], axis=0
            )
            pieces.append(dot(eye, tall, NT))
        return pieces

    def place_weights(n, pieces):
        extra = 9 * pack
        turned = []
        for t, b0 in enumerate(pieces):
            b1, b2, b3 = (pltpu.roll(b0, i * chan, 1) for i in (1, 2, 3))
            turned.append((b0, b1, b2, b3))
            mid = jnp.where(quad >= 2, b2, 0.0).astype(BF16)
            a0, a1 = b0.astype(BF16), b1.astype(BF16)
            low = jnp.where(quad < 2, b3, 0.0).astype(BF16)
            high = jnp.where(quad == 3, b3, 0.0).astype(BF16)
            for h, blocks in enumerate(((low, a0, a1, mid), (a0, a1, mid, high))):
                for y, block in enumerate(blocks):
                    wcat[n, h, y * chan : (y + 1) * chan, t * pack : (t + 1) * pack] = block

        def gather(off, q):
            value = jnp.zeros((chan, pack), F32)
            for t in range(4 * q, min(4 * q + 4, 9)):
                value = jnp.where(quad == t % 4, turned[t][(t - off) % 4], value)
            return value.astype(BF16)

        for q in range(3):
            at = slice(extra + q * pack, extra + (q + 1) * pack)
            last = gather(2, q)
            wcat[n, 0, 3 * chan : 4 * chan, at] = last
            wcat[n, 1, 2 * chan : 3 * chan, at] = last
            wcat[n, 1, 3 * chan : 4 * chan, at] = gather(1, q)

    for n in range(4):
        at = slice(9 * pack, 12 * pack)
        wcat[n, 0, : 3 * chan, at] = jnp.zeros((3 * chan, 3 * pack), BF16)
        wcat[n, 1, : 2 * chan, at] = jnp.zeros((2 * chan, 3 * pack), BF16)

    def scatter_terms(j):
        def send(to_dp):
            to = to_dp - own_low
            inside = (to >= 0) & (to < owners)

            @pl.when(inside & ((gz != own_gz) | (dp != to_dp)))
            def _():
                pltpu.make_async_remote_copy(
                    src_ref=packed.at[j, to],
                    dst_ref=arrived.at[j, me],
                    send_sem=rs_send.at[j],
                    recv_sem=rs_recv.at[j],
                    device_id={"gz": own_gz, "dp": to_dp},
                    device_id_type=MESH,
                ).start()

        if count <= UNROLL_UP_TO:
            for a in far_first:
                base = lax.rem(dp_out + a, outer) * inner_count
                for b in reversed(range(inner_count)):
                    send(base + lax.rem(dp_in + b, inner_count))
        else:
            for i in range(owners):
                send(lax.rem(dp + i, owners) + own_low)

        @pl.when(owner)
        def _():
            arrived[j, me] = packed[j, rank]

    def wait_for(ref, sem):
        pltpu.make_async_copy(ref, ref, sem).wait()

    def gather_terms(j):
        @pl.when(owner)
        def _():
            wait_for(arrived.at[j, pl.ds(0, count - 1)], rs_recv.at[j])
            full[j, rank] = jnp.sum(arrived[j].astype(F32), axis=0).astype(BF16)

            def send(slot, to_gz, to_dp):
                pltpu.make_async_remote_copy(
                    src_ref=full.at[j, rank],
                    dst_ref=full.at[j, rank],
                    send_sem=ag_send.at[j],
                    recv_sem=ag_recv.at[j],
                    device_id={"gz": to_gz, "dp": to_dp},
                    device_id_type=MESH,
                ).start()

            each_peer(send)

    def finish_terms(j):
        tiles = packed.shape[2]

        @pl.when(owner)
        def _():
            wait_for(full.at[j, pl.ds(0, owners - 1)], ag_recv.at[j])
            wait_for(packed.at[j, pl.ds(0, owners - 1)], rs_send.at[j])
            wait_for(arrived.at[j, pl.ds(0, count - 1)], ag_send.at[j])

        @pl.when(jnp.logical_not(owner))
        def _():
            wait_for(full.at[j, pl.ds(0, owners)], ag_recv.at[j])
            wait_for(packed.at[j, pl.ds(0, owners)], rs_send.at[j])

        groups = chan // 8
        tile = lambda k: full[j, k // tiles, k % tiles].astype(F32)
        for o in range(groups):
            at = slice(8 * o, 8 * o + 8)
            for kx in range(3):
                for g in range(2):
                    both = tile((kx * groups + o) * 2 + g)
                    for i in range(4):
                        grads_ref[j, (4 * g + i) * 3 + kx, at] = both[:, i * chan : (i + 1) * chan]
            rest = tile(6 * groups + o)
            for kx in range(3):
                grads_ref[j, 24 + kx, at] = rest[:, kx * chan : (kx + 1) * chan]

    pr, pc = iota((3 * chan, 8 * chan), 0), iota((3 * chan, 8 * chan), 1)
    choose = one_hot(pc == (2 - pr // chan) * 2 * chan + pr % chan)

    halves = [range(height // 4), range(height // 4, height // 2)]

    def products(s, s_grad, planes):
        cuts = [planes[i : i + 2] for i in range(0, len(planes), 2)]

        def source(pairs, plane, rel):
            cells = []
            for cut in cuts:
                for m in pairs:
                    y = 2 * m + rel
                    for p in cut:
                        if 0 <= y < height:
                            cells.append(s[1, p + plane, y * chan : (y + 1) * chan])
                        else:
                            cells.append(jnp.zeros((chan, width), BF16))
            return lanes(cells)

        def grad(pairs, col):
            return lanes(
                [
                    s_grad[col, p + 1, 2 * m * chan : (2 * m + 2) * chan]
                    for cut in cuts
                    for m in pairs
                    for p in cut
                ]
            )

        values = []
        for pairs in halves:
            streamed = [source(pairs, plane, rel) for plane in range(3) for rel in range(-1, 3)]
            held = [grad(pairs, col) for col in (0, 1, 2, 1)]
            values.append(
                dot(jnp.concatenate(streamed, axis=0), jnp.concatenate(held, axis=0), NT)
            )
        return values

    def add_terms(j, s, s_grad, planes, first=False):
        one, two = products(s, s_grad, planes)
        value = one * factor + two * factor
        sums_acc[j] = value if first else sums_acc[j] + value

    def end_terms(j, s, s_grad, planes):
        one, two = products(s, s_grad, planes)

        def block(at, i):
            cells = slice(i * pack, (i + 1) * pack)
            rest = one[at : at + chan, cells] * factor + two[at : at + chan, cells] * factor
            return sums_acc[j, at : at + chan, cells] + rest

        blocks = []
        for plane in range(3):
            for off in range(3):
                at = (plane * 4 + off) * chan
                blocks.append(
                    lanes(
                        [
                            block(at, i) + pltpu.roll(block(at + chan, i), 3 * chan, 1)
                            for i in range(2)
                        ]
                    ).astype(BF16)
                )
        blocks.append(jnp.zeros((3 * chan, 8 * chan), BF16))
        turned = dot(choose, jnp.concatenate(blocks, axis=0), NT)
        tail = turned[:, 2 * pack :]
        tail = (
            tail[:chan]
            + pltpu.roll(tail[chan : 2 * chan], chan, 1)
            + pltpu.roll(tail[2 * chan :], 2 * chan, 1)
        )
        tiles = packed.shape[2]
        sources = [
            turned[8 * i : 8 * i + 8, g * pack : (g + 1) * pack]
            for i in range(3 * chan // 8)
            for g in range(2)
        ] + [tail[8 * i : 8 * i + 8] for i in range(chan // 8)]
        for t, tile in enumerate(sources):
            packed[j, t // tiles, t % tiles] = tile.astype(BF16)

    if owners * packed.shape[2] > 28:
        packed[...] = jnp.zeros_like(packed)

    def first_layer(planes):
        for h in range(2):
            at = pl.ds(h * part_rows, part_rows)
            for p, pre in zip(planes, conv(0, s_in, planes, h)):
                sig = sigmoid(pre)
                slope[p, at] = sig * (1.0 + pre * (1.0 - sig))
                put(s_hid, p + 1, h, pre * sig)

    def second_layer(planes):
        cots = load(cot_ref, planes)
        for h in range(2):
            for p, pre, cot in zip(planes, conv(1, s_hid, planes, h), cots):
                sig = sigmoid(pre)
                cot = cot[h * part_rows : (h + 1) * part_rows]
                put(s_g2, p + 1, h, cot * (sig * (1.0 + pre * (1.0 - sig))))

    def second_back(planes):
        for h in range(2):
            at = pl.ds(h * part_rows, part_rows)
            for p, value in zip(planes, conv(2, s_g2, planes, h)):
                put(s_g1, p + 1, h, value * slope[p, at])

    def first_back(planes):
        value = jnp.concatenate(
            [lanes(conv(3, s_g1, planes, h)).astype(BF16) for h in range(2)], axis=0
        )
        for p, part in zip(planes, split(dot(perm[1], value), planes)):
            out_ref[:, p] = part.reshape(chan, height, width).astype(BF16)

    ring = lambda k: sorted({k, depth - 1 - k})

    def pairs_from(k):
        planes = list(range(k, depth - k))
        return [planes[i : i + 2] for i in range(0, len(planes), 2)]

    loads[0].wait()
    loads[1].wait()
    place_weights(0, forward(w1_ref))
    for planes in groups:
        for p, value in zip(planes, load(x_ref, planes)):
            for h in range(2):
                put(s_in, p + 1, h, value[h * part_rows : (h + 1) * part_rows])
    for copy in loads[2:]:
        copy.wait()
    for i, planes in enumerate(pairs_from(1)):
        first_layer(planes)
        if i == 0:
            place_weights(1, forward(w2_ref))
    for planes in pairs_from(2):
        second_layer(planes)
    pl.semaphore_wait(barrier, count - 1)
    send_halo(0)
    place_weights(2, backward(w2_ref))
    add_terms(1, s_hid, s_g2, [p for planes in pairs_from(2) for p in planes], True)
    for planes in pairs_from(3):
        second_back(planes)
    take_halo(0)
    first_layer(ring(0))
    send_halo(1)
    second_layer(ring(1))
    second_back(ring(2))
    take_halo(1)
    second_layer(ring(0))
    send_halo(2)
    add_terms(0, s_in, s_g1, [p for planes in pairs_from(2) for p in planes], True)
    second_back(ring(1))
    end_terms(1, s_hid, s_g2, ring(1) + ring(0))
    scatter_terms(1)
    take_halo(2)
    second_back(ring(0))
    send_halo(3)
    end_terms(0, s_in, s_g1, ring(1) + ring(0))
    scatter_terms(0)
    place_weights(3, backward(w1_ref))
    for planes in groups[1:]:
        first_back(planes)
    take_halo(3)
    first_back(ring(0))
    gather_terms(1)
    gather_terms(0)
    finish_terms(1)
    finish_terms(0)

    for n in range(4):

        @pl.when(gz < gz_count - 1)
        def _():
            up_copy(n).wait_send()

        @pl.when(gz > 0)
        def _():
            down_copy(n).wait_send()


def write_out(out_ref, grads_ref, out_hbm, g1_hbm, g2_hbm, sems):
    moves = ((out_ref, out_hbm), (grads_ref.at[0], g1_hbm), (grads_ref.at[1], g2_hbm))
    copies = [pltpu.make_async_copy(src, dst, sems.at[i]) for i, (src, dst) in enumerate(moves)]
    for copy in copies:
        copy.start()
    for copy in copies:
        copy.wait()


def solution(mesh):
    gz_count, dp_count = mesh.shape["gz"], mesh.shape["dp"]
    count = gz_count * dp_count

    def local(inputs, kernel_one, kernel_two, cotangent):
        _, chan, depth, height, width = inputs.shape
        rows = chan * height
        cells = dp_count * gz_count * depth * height * width
        own_count = dp_count // 2 if dp_count % 4 == 0 else dp_count
        own_low = (dp_count - own_count) // 2
        tiles = -(-28 // own_count)
        owners = -(-28 // tiles)
        taps = lambda k: k.transpose(2, 3, 4, 0, 1).reshape(27, chan, chan)
        slab = pltpu.VMEM((3, depth + 2, rows, width), BF16)
        vmem = pl.BlockSpec(memory_space=pltpu.VMEM)
        anywhere = pl.BlockSpec(memory_space=pl.ANY)
        out, grads = pl.pallas_call(
            functools.partial(kernel, (gz_count, dp_count, owners, (gz_count - 1, own_low)), 1.0 / math.sqrt(cells)),
            out_shape=(
                pltpu.VMEM((chan, depth, height, width), BF16),
                pltpu.VMEM((2, 27, chan, chan), F32),
            ),
            in_specs=[anywhere] * 4,
            out_specs=(vmem, vmem),
            scratch_shapes=[
                pltpu.VMEM((chan, depth, height, width), BF16),
                pltpu.VMEM((27, chan, chan), BF16),
                pltpu.VMEM((27, chan, chan), BF16),
                pltpu.VMEM((chan, depth, height, width), BF16),
                slab,
                slab,
                slab,
                slab,
                pltpu.VMEM((4, 2, rows // 2, 12 * 4 * chan), BF16),
                pltpu.VMEM((depth, rows, width), F32),
                pltpu.VMEM((2, rows, rows), BF16),
                pltpu.VMEM((2, 12 * chan, 8 * chan), F32),
                pltpu.VMEM((2, owners, tiles, 8, 128), BF16),
                pltpu.VMEM((2, count, tiles, 8, 128), BF16),
                pltpu.VMEM((2, owners, tiles, 8, 128), BF16),
                pltpu.SemaphoreType.DMA((4, 2)),
                pltpu.SemaphoreType.DMA((4, 2)),
                pltpu.SemaphoreType.DMA((2,)),
                pltpu.SemaphoreType.DMA((2,)),
                pltpu.SemaphoreType.DMA((2,)),
                pltpu.SemaphoreType.DMA((2,)),
                pltpu.SemaphoreType.DMA((4,)),
            ],
            compiler_params=pltpu.CompilerParams(collective_id=0, has_side_effects=True),
        )(inputs[0], taps(kernel_one), taps(kernel_two), cotangent[0])
        out, grads = (pltpu.with_memory_space_constraint(v, pltpu.VMEM) for v in (out, grads))
        out, g1, g2 = pl.pallas_call(
            write_out,
            out_shape=(
                jax.ShapeDtypeStruct((chan, depth, height, width), BF16),
                jax.ShapeDtypeStruct((27, chan, chan), F32),
                jax.ShapeDtypeStruct((27, chan, chan), F32),
            ),
            in_specs=[vmem] * 2,
            out_specs=(anywhere,) * 3,
            scratch_shapes=[pltpu.SemaphoreType.DMA((3,))],
        )(out, grads)
        back = lambda g: g.reshape(3, 3, 3, chan, chan).transpose(3, 4, 0, 1, 2)
        return out[None], back(g1), back(g2)

    return jax.shard_map(
        local,
        mesh=mesh,
        in_specs=(P("dp", None, "gz", None, None), P(), P(), P("dp", None, "gz", None, None)),
        out_specs=(P("dp", None, "gz", None, None), P(), P()),
        check_vma=False,
    )
```
